32 devices in a mesh: depth: 4 (over z), imgx: 4 (over y, core), imgy: 2 (over x).
Axes of the slice: x: 2, y: 2, z: 4, core: 2. Of those that a mesh axis runs over, the one named last changes fastest.
Arguments:
- emissivity: bfloat16 [32, 512, 256], P('depth', 'imgx', 'imgy'), may hold values from 0.099609375 to 10
- bin_index: int32 [32, 512, 256], P('depth', 'imgx', 'imgy'), may hold values from 0 to 127
- color_table: bfloat16 [4, 128], replicated, may hold values from 0.049804688 to 1
- brick_order: int32 [4], replicated, may hold values from 0 to 3, each once
Outputs:
- image: float32 [4, 512, 256], P(None, 'imgx', 'imgy')
The draws below stay inside these ranges and needn't reach their ends.
Inputs may be any that keep to these rules, and one draw needn't show every extreme that they name: brick_order names every brick index once.
All inputs are finite; a program needn't handle non-finite values.
Results may differ from the reference program's by a relative error of at most 0.0003.
Values sent between devices are 32-bit elements; how exact they have to be, the bound alone decides.
A program may use at most 64 MiB of HBM per device.

```python
import math
import jax
import jax.numpy as jnp
from jax import lax

DZ = 8
BINS = 128
NZ = 32
NX = 512
NY = 256
N_DEPTH = 4


def set_ends(entries, rng, least, high):
    extent = entries.shape
    index_at = [jax.random.randint(jax.random.fold_in(rng, axis), (), 0, extent[axis]) for axis in range(len(extent))]
    entries = entries.at[tuple(index_at)].set(least)
    longest = extent.index(max(extent))
    index_at[longest] = (index_at[longest] + 1) % extent[longest]
    return entries.at[tuple(index_at)].set(high)


def level_of(rng, shape, split, least, largest):
    level = 1.0
    for dim, shards_of in split:
        heights = jax.random.uniform(jax.random.fold_in(jax.random.fold_in(rng, 6), dim), (shards_of,), jnp.float32, least / len(split), largest / len(split))
        level = level * jnp.repeat(jnp.exp(heights), shape[dim] // shards_of).reshape((-1,) + (1,) * (len(shape) - 1 - dim))
    return level


def setup_inputs(seed: int = 0) -> dict:
    keys = jax.random.split(jax.random.key(seed), 5)
    emissivity = jnp.clip(jnp.exp(math.log(10.0) - 4.609084 * jax.random.uniform(keys[0], (NZ, NX, NY), jnp.float32) ** level_of(keys[0], (NZ, NX, NY), ((0, 4), (1, 4), (2, 2)), -0.2, 0.2)), 0.099609375, 10.0).astype(jnp.bfloat16)
    bin_index = set_ends(jax.random.randint(keys[1], (NZ, NX, NY), 0, BINS), jax.random.fold_in(keys[1], 1), 0, BINS - 1).astype(jnp.int32)
    color_table = jnp.clip(jnp.exp(jax.random.uniform(keys[2], (4, BINS), jnp.float32, math.log(0.049804688), math.log(1.0))), 0.049804688, 1.0).astype(jnp.bfloat16)
    brick_order = jax.random.permutation(keys[3], N_DEPTH).astype(jnp.int32)
    return dict(emissivity=emissivity, bin_index=bin_index, color_table=color_table, brick_order=brick_order)


def brick_partial(bright_cells, bin_cells, color_table, ray_step):
    looked = color_table.astype(jnp.float32)[:, bin_cells]
    bright = bright_cells.astype(jnp.float32)
    glow_rgb = bright[None] * looked[0:3]
    absorb_rate = bright * looked[3]
    depth_in = jnp.cumsum(absorb_rate, axis=0) - absorb_rate
    light_in = jnp.exp(-ray_step * depth_in)
    color_sum = jnp.sum(ray_step * glow_rgb * light_in[None], axis=1)
    passed = jnp.exp(-ray_step * jnp.sum(absorb_rate, axis=0))
    return color_sum, passed


def reference(emissivity, bin_index, color_table, brick_order):
    ray_step = 2.0 / NZ

    def advance(state_pair, brick_id):
        color_acc, through = state_pair
        start_cell = (brick_id * DZ).astype(jnp.int32)
        brick_cells = lax.dynamic_slice_in_dim(emissivity, start_cell, DZ, 0)
        brick_bins = lax.dynamic_slice_in_dim(bin_index, start_cell, DZ, 0)
        color_sum, passed = brick_partial(brick_cells, brick_bins, color_table, ray_step)
        return (color_acc + through[None] * color_sum, through * passed), None

    start_state = (jnp.zeros((3, NX, NY), jnp.float32), jnp.ones((NX, NY), jnp.float32))
    final_state, _ = lax.scan(advance, start_state, brick_order)
    color_acc, through = final_state
    return jnp.concatenate([color_acc, (1.0 - through)[None]], 0)
```

```python
import functools

import jax
import jax.numpy as jnp
from jax import lax
from jax.experimental import pallas as pl
from jax.experimental.pallas import tpu as pltpu
from jax.sharding import PartitionSpec as P

MESH = pl.DeviceIdType.MESH
BLOCK = 16
LANES = 128


def look(channel_tables, bins):
    slabs = len(channel_tables[0])
    if slabs == 1:
        return [jnp.take_along_axis(t[0], bins, axis=1, mode="promise_in_bounds") for t in channel_tables]
    within = bins % LANES
    slab_of = bins // LANES
    out = []
    for t in channel_tables:
        value = jnp.take_along_axis(t[0], within, axis=1, mode="promise_in_bounds")
        for s in range(1, slabs):
            other = jnp.take_along_axis(t[s], within, axis=1, mode="promise_in_bounds")
            value = jnp.where(slab_of == s, other, value)
        out.append(value)
    return out


def scaled_tables(table_ref, ray_step):
    table = table_ref[...].astype(jnp.float32) * ray_step
    slabs = table.shape[1] // LANES
    return [
        [jnp.broadcast_to(table[c : c + 1, s * LANES : (s + 1) * LANES], (BLOCK, LANES)) for s in range(slabs)]
        for c in range(4)
    ]


def march(tables, emis_ref, bins_ref, start):
    cells = emis_ref.shape[0]
    rows = pl.ds(start, BLOCK)
    color = [None] * 3
    depth_in = None
    for z in range(cells):
        bright = emis_ref[z, rows, :].astype(jnp.float32)
        looked = look(tables, bins_ref[z, rows, :])
        rate = bright * looked[3]
        if depth_in is None:
            color = [bright * looked[c] for c in range(3)]
            depth_in = rate
        else:
            seen = bright * jnp.exp(-depth_in)
            color = [color[c] + seen * looked[c] for c in range(3)]
            depth_in = depth_in + rate
    return color + [jnp.exp(-depth_in)]


def fused(n, ray_step, emis_hbm, bins_hbm, table_ref, order_ref, out_ref,
          emis, bins, outgoing, arrived, mine, in_sem, send_sem, recv_sem, give_sem, take_sem):
    me = lax.axis_index("depth")
    rows = mine.shape[1]
    hops = sorted(range(1, n), key=lambda h: (-min(h, n - h), h)) + [0]

    def at_hop(h):
        return lax.rem(me + h, n)

    def span(d):
        return pl.ds(pl.multiple_of(d * rows, BLOCK), rows)

    loads = []
    for i, h in enumerate(hops):
        dest = span(at_hop(h))
        pair = (
            pltpu.make_async_copy(emis_hbm.at[:, dest, :], emis.at[i], in_sem.at[2 * i]),
            pltpu.make_async_copy(bins_hbm.at[:, dest, :], bins.at[i], in_sem.at[2 * i + 1]),
        )
        for c in pair:
            c.start()
        loads.append(pair)

    barrier = pltpu.get_barrier_semaphore()
    for h in range(1, n):
        pl.semaphore_signal(barrier, inc=1, device_id={"depth": at_hop(h)}, device_id_type=MESH)

    tables = scaled_tables(table_ref, ray_step)
    sends = []
    for i, h in enumerate(hops):
        for c in loads[i]:
            c.wait()
        for r in range(0, rows, BLOCK):
            part = march(tables, emis.at[i], bins.at[i], r)
            for c in range(4):
                if h == 0:
                    arrived[me, c, pl.ds(r, BLOCK), :] = part[c]
                else:
                    outgoing[i, c, pl.ds(r, BLOCK), :] = part[c]
        if h != 0:
            if i == 0:
                pl.semaphore_wait(barrier, n - 1)
            copy = pltpu.make_async_remote_copy(
                src_ref=outgoing.at[i],
                dst_ref=arrived.at[me],
                send_sem=send_sem.at[i],
                recv_sem=recv_sem.at[i],
                device_id={"depth": at_hop(h)},
                device_id_type=MESH,
            )
            copy.start()
            sends.append(copy)
    for copy in sends:
        copy.wait_recv()

    for r in range(0, rows, BLOCK):
        at = pl.ds(r, BLOCK)
        first = order_ref[0]
        color = [arrived[first, c, at, :] for c in range(3)]
        through = arrived[first, 3, at, :]
        for k in range(1, n):
            b = order_ref[k]
            color = [color[c] + through * arrived[b, c, at, :] for c in range(3)]
            through = through * arrived[b, 3, at, :]
        for c in range(3):
            mine[c, at, :] = color[c]
        mine[3, at, :] = 1.0 - through

    gives = []
    for i, h in enumerate(hops[:-1]):
        copy = pltpu.make_async_remote_copy(
            src_ref=mine,
            dst_ref=out_ref.at[:, span(me), :],
            send_sem=give_sem.at[i],
            recv_sem=take_sem.at[i],
            device_id={"depth": at_hop(h)},
            device_id_type=MESH,
        )
        copy.start()
        gives.append(copy)
    out_ref[:, span(me), :] = mine[...]
    for copy in sends:
        copy.wait_send()
    for copy in gives:
        copy.wait()


def fused_call(emissivity, bin_index, color_table, brick_order, n, ray_step):
    cells, cols_x, cols_y = emissivity.shape
    rows = cols_x // n
    return pl.pallas_call(
        functools.partial(fused, n, ray_step),
        out_shape=jax.ShapeDtypeStruct((4, cols_x, cols_y), jnp.float32),
        in_specs=[
            pl.BlockSpec(memory_space=pltpu.HBM),
            pl.BlockSpec(memory_space=pltpu.HBM),
            pl.BlockSpec(memory_space=pltpu.VMEM),
            pl.BlockSpec(memory_space=pltpu.SMEM),
        ],
        out_specs=pl.BlockSpec(memory_space=pltpu.VMEM),
        scratch_shapes=[
            pltpu.VMEM((n, cells, rows, cols_y), jnp.bfloat16),
            pltpu.VMEM((n, cells, rows, cols_y), jnp.int32),
            pltpu.VMEM((n - 1, 4, rows, cols_y), jnp.float32),
            pltpu.VMEM((n, 4, rows, cols_y), jnp.float32),
            pltpu.VMEM((4, rows, cols_y), jnp.float32),
            pltpu.SemaphoreType.DMA((2 * n,)),
            pltpu.SemaphoreType.DMA((n - 1,)),
            pltpu.SemaphoreType.DMA((n - 1,)),
            pltpu.SemaphoreType.DMA((n - 1,)),
            pltpu.SemaphoreType.DMA((n - 1,)),
        ],
        compiler_params=pltpu.CompilerParams(collective_id=0, has_side_effects=True),
    )(emissivity, bin_index, color_table, brick_order)


def march_kernel(ray_step, emis_ref, bins_ref, table_ref, out_ref):
    tables = scaled_tables(table_ref, ray_step)

    @pl.loop(0, emis_ref.shape[1] // BLOCK)
    def _(r):
        start = pl.multiple_of(r * BLOCK, BLOCK)
        part = march(tables, emis_ref, bins_ref, start)
        for c in range(4):
            out_ref[c, pl.ds(start, BLOCK), :] = part[c]


def spread(emissivity, bin_index, color_table, brick_order, n, ray_step):
    cells, cols_x, cols_y = emissivity.shape
    piece_len = cols_x * cols_y // n
    stacked = pl.pallas_call(
        functools.partial(march_kernel, ray_step),
        out_shape=jax.ShapeDtypeStruct((4, cols_x, cols_y), jnp.float32),
        in_specs=[pl.BlockSpec(memory_space=pltpu.VMEM)] * 3,
        out_specs=pl.BlockSpec(memory_space=pltpu.VMEM),
    )(emissivity, bin_index, color_table)
    stacked = stacked.reshape(1, 4, n, piece_len).transpose(2, 0, 1, 3).reshape(n, 4, piece_len)
    received = lax.all_to_all(stacked, "depth", split_axis=0, concat_axis=0, tiled=True)
    ordered = jnp.take(received, brick_order, axis=0)
    color, through = ordered[0, 0:3], ordered[0, 3]
    for k in range(1, n):
        color = color + through * ordered[k, 0:3]
        through = through * ordered[k, 3]
    piece = jnp.concatenate([color, (1.0 - through)[None]], 0)
    return lax.all_gather(piece, "depth", axis=1, tiled=True).reshape(4, cols_x, cols_y)


def on_device(emissivity, bin_index, color_table, brick_order):
    cells, cols_x, cols_y = emissivity.shape
    n = lax.axis_size("depth")
    ray_step = 2.0 / (cells * n)
    piecewise = cols_x % (n * BLOCK) == 0
    form = fused_call if piecewise else spread
    return form(emissivity, bin_index, color_table, brick_order, n, ray_step)


def solution(mesh):
    return jax.shard_map(
        on_device,
        mesh=mesh,
        in_specs=(P("depth", "imgx", "imgy"), P("depth", "imgx", "imgy"), P(), P()),
        out_specs=P(None, "imgx", "imgy"),
        check_vma=False,
    )
```

```python
import functools

import jax
import jax.numpy as jnp
from jax import lax
from jax.experimental import pallas as pl
from jax.experimental.pallas import tpu as pltpu
from jax.sharding import PartitionSpec as P

MESH = pl.DeviceIdType.MESH
BLOCK = 16
LANES = 128


def look(channel_tables, bins):
    slabs = len(channel_tables[0])
    if slabs == 1:
        return [jnp.take_along_axis(t[0], bins, axis=1, mode="promise_in_bounds") for t in channel_tables]
    within = bins % LANES
    slab_of = bins // LANES
    out = []
    for t in channel_tables:
        value = jnp.take_along_axis(t[0], within, axis=1, mode="promise_in_bounds")
        for s in range(1, slabs):
            other = jnp.take_along_axis(t[s], within, axis=1, mode="promise_in_bounds")
            value = jnp.where(slab_of == s, other, value)
        out.append(value)
    return out


def scaled_tables(table_ref, ray_step):
    table = table_ref[...].astype(jnp.float32) * ray_step
    slabs = table.shape[1] // LANES
    return [
        [jnp.broadcast_to(table[c : c + 1, s * LANES : (s + 1) * LANES], (BLOCK, LANES)) for s in range(slabs)]
        for c in range(4)
    ]


def march(tables, emis_ref, bins_ref, start):
    cells = emis_ref.shape[0]
    rows = pl.ds(start, BLOCK)
    color = [None] * 3
    depth_in = None
    for z in range(cells):
        bright = emis_ref[z, rows, :].astype(jnp.float32)
        looked = look(tables, bins_ref[z, rows, :])
        rate = bright * looked[3]
        if depth_in is None:
            color = [bright * looked[c] for c in range(3)]
            depth_in = rate
        else:
            seen = bright * jnp.exp(-depth_in)
            color = [color[c] + seen * looked[c] for c in range(3)]
            depth_in = depth_in + rate
    return color + [jnp.exp(-depth_in)]


def fused(n, ray_step, emis_hbm, bins_hbm, table_ref, order_ref, out_ref,
          emis, bins, outgoing, arrived, mine, in_sem, send_sem, recv_sem, give_sem, take_sem):
    me = lax.axis_index("depth")
    rows = mine.shape[1]
    hops = sorted(range(1, n), key=lambda h: (-min(h, n - h), h)) + [0]

    def at_hop(h):
        return lax.rem(me + h, n)

    def span(d):
        return pl.ds(pl.multiple_of(d * rows, BLOCK), rows)

    loads = []
    for i, h in enumerate(hops):
        dest = span(at_hop(h))
        pair = (
            pltpu.make_async_copy(emis_hbm.at[:, dest, :], emis.at[i], in_sem.at[2 * i]),
            pltpu.make_async_copy(bins_hbm.at[:, dest, :], bins.at[i], in_sem.at[2 * i + 1]),
        )
        for c in pair:
            c.start()
        loads.append(pair)

    barrier = pltpu.get_barrier_semaphore()
    for h in range(1, n):
        pl.semaphore_signal(barrier, inc=1, device_id={"depth": at_hop(h)}, device_id_type=MESH)

    tables = scaled_tables(table_ref, ray_step)
    sends = []
    for i, h in enumerate(hops):
        for c in loads[i]:
            c.wait()
        for r in range(0, rows, BLOCK):
            part = march(tables, emis.at[i], bins.at[i], r)
            for c in range(4):
                if h == 0:
                    arrived[me, c, pl.ds(r, BLOCK), :] = part[c]
                else:
                    outgoing[i, c, pl.ds(r, BLOCK), :] = part[c]
        if h != 0:
            if i == 0:
                pl.semaphore_wait(barrier, n - 1)
            copy = pltpu.make_async_remote_copy(
                src_ref=outgoing.at[i],
                dst_ref=arrived.at[me],
                send_sem=send_sem.at[i],
                recv_sem=recv_sem.at[i],
                device_id={"depth": at_hop(h)},
                device_id_type=MESH,
            )
            copy.start()
            sends.append(copy)
    for copy in sends:
        copy.wait_recv()

    for r in range(0, rows, BLOCK):
        at = pl.ds(r, BLOCK)
        first = order_ref[0]
        color = [arrived[first, c, at, :] for c in range(3)]
        through = arrived[first, 3, at, :]
        for k in range(1, n):
            b = order_ref[k]
            color = [color[c] + through * arrived[b, c, at, :] for c in range(3)]
            through = through * arrived[b, 3, at, :]
        for c in range(3):
            mine[c, at, :] = color[c]
        mine[3, at, :] = 1.0 - through

    gives = []
    for i, h in enumerate(hops[:-1]):
        copy = pltpu.make_async_remote_copy(
            src_ref=mine,
            dst_ref=out_ref.at[:, span(me), :],
            send_sem=give_sem.at[i],
            recv_sem=take_sem.at[i],
            device_id={"depth": at_hop(h)},
            device_id_type=MESH,
        )
        copy.start()
        gives.append(copy)
    out_ref[:, span(me), :] = mine[...]
    for copy in sends:
        copy.wait_send()
    for copy in gives:
        copy.wait()


def fused_call(emissivity, bin_index, color_table, brick_order, n, ray_step):
    cells, cols_x, cols_y = emissivity.shape
    rows = cols_x // n
    return pl.pallas_call(
        functools.partial(fused, n, ray_step),
        out_shape=pltpu.VMEM((4, cols_x, cols_y), jnp.float32),
        in_specs=[
            pl.BlockSpec(memory_space=pltpu.HBM),
            pl.BlockSpec(memory_space=pltpu.HBM),
            pl.BlockSpec(memory_space=pltpu.VMEM),
            pl.BlockSpec(memory_space=pltpu.SMEM),
        ],
        out_specs=pl.BlockSpec(memory_space=pltpu.VMEM),
        scratch_shapes=[
            pltpu.VMEM((n, cells, rows, cols_y), jnp.bfloat16),
            pltpu.VMEM((n, cells, rows, cols_y), jnp.int32),
            pltpu.VMEM((n - 1, 4, rows, cols_y), jnp.float32),
            pltpu.VMEM((n, 4, rows, cols_y), jnp.float32),
            pltpu.VMEM((4, rows, cols_y), jnp.float32),
            pltpu.SemaphoreType.DMA((2 * n,)),
            pltpu.SemaphoreType.DMA((n - 1,)),
            pltpu.SemaphoreType.DMA((n - 1,)),
            pltpu.SemaphoreType.DMA((n - 1,)),
            pltpu.SemaphoreType.DMA((n - 1,)),
        ],
        compiler_params=pltpu.CompilerParams(collective_id=0, has_side_effects=True),
    )(emissivity, bin_index, color_table, brick_order)


def march_kernel(ray_step, emis_ref, bins_ref, table_ref, out_ref):
    tables = scaled_tables(table_ref, ray_step)

    @pl.loop(0, emis_ref.shape[1] // BLOCK)
    def _(r):
        start = pl.multiple_of(r * BLOCK, BLOCK)
        part = march(tables, emis_ref, bins_ref, start)
        for c in range(4):
            out_ref[c, pl.ds(start, BLOCK), :] = part[c]


def spread(emissivity, bin_index, color_table, brick_order, n, ray_step):
    cells, cols_x, cols_y = emissivity.shape
    piece_len = cols_x * cols_y // n
    stacked = pl.pallas_call(
        functools.partial(march_kernel, ray_step),
        out_shape=jax.ShapeDtypeStruct((4, cols_x, cols_y), jnp.float32),
        in_specs=[pl.BlockSpec(memory_space=pltpu.VMEM)] * 3,
        out_specs=pl.BlockSpec(memory_space=pltpu.VMEM),
    )(emissivity, bin_index, color_table)
    stacked = stacked.reshape(1, 4, n, piece_len).transpose(2, 0, 1, 3).reshape(n, 4, piece_len)
    received = lax.all_to_all(stacked, "depth", split_axis=0, concat_axis=0, tiled=True)
    ordered = jnp.take(received, brick_order, axis=0)
    color, through = ordered[0, 0:3], ordered[0, 3]
    for k in range(1, n):
        color = color + through * ordered[k, 0:3]
        through = through * ordered[k, 3]
    piece = jnp.concatenate([color, (1.0 - through)[None]], 0)
    return lax.all_gather(piece, "depth", axis=1, tiled=True).reshape(4, cols_x, cols_y)


def on_device(emissivity, bin_index, color_table, brick_order):
    cells, cols_x, cols_y = emissivity.shape
    n = lax.axis_size("depth")
    ray_step = 2.0 / (cells * n)
    piecewise = cols_x % (n * BLOCK) == 0
    form = fused_call if piecewise else spread
    return form(emissivity, bin_index, color_table, brick_order, n, ray_step)


def solution(mesh):
    return jax.shard_map(
        on_device,
        mesh=mesh,
        in_specs=(P("depth", "imgx", "imgy"), P("depth", "imgx", "imgy"), P(), P()),
        out_specs=P(None, "imgx", "imgy"),
        check_vma=False,
    )
```

```python
import functools

import jax
import jax.numpy as jnp
from jax import lax
from jax.experimental import pallas as pl
from jax.experimental.pallas import tpu as pltpu
from jax.sharding import PartitionSpec as P

MESH = pl.DeviceIdType.MESH
BLOCK = 16
LANES = 128


def look(channel_tables, bins):
    slabs = len(channel_tables[0])
    if slabs == 1:
        return [jnp.take_along_axis(t[0], bins, axis=1, mode="promise_in_bounds") for t in channel_tables]
    within = bins % LANES
    slab_of = bins // LANES
    out = []
    for t in channel_tables:
        value = jnp.take_along_axis(t[0], within, axis=1, mode="promise_in_bounds")
        for s in range(1, slabs):
            other = jnp.take_along_axis(t[s], within, axis=1, mode="promise_in_bounds")
            value = jnp.where(slab_of == s, other, value)
        out.append(value)
    return out


def scaled_tables(table_ref, ray_step):
    table = table_ref[...].astype(jnp.float32) * ray_step
    slabs = table.shape[1] // LANES
    return [
        [jnp.broadcast_to(table[c : c + 1, s * LANES : (s + 1) * LANES], (BLOCK, LANES)) for s in range(slabs)]
        for c in range(4)
    ]


def march(tables, emis_ref, bins_ref, start):
    cells = emis_ref.shape[0]
    rows = pl.ds(start, BLOCK)
    color = [None] * 3
    depth_in = None
    for z in range(cells):
        bright = emis_ref[z, rows, :].astype(jnp.float32)
        looked = look(tables, bins_ref[z, rows, :])
        rate = bright * looked[3]
        if depth_in is None:
            color = [bright * looked[c] for c in range(3)]
            depth_in = rate
        else:
            seen = bright * jnp.exp(-depth_in)
            color = [color[c] + seen * looked[c] for c in range(3)]
            depth_in = depth_in + rate
    return color + [jnp.exp(-depth_in)]


def fused(n, ray_step, emis_hbm, bins_hbm, table_ref, order_ref, out_ref,
          emis, bins, outgoing, arrived, mine, in_sem, send_sem, recv_sem, give_sem, take_sem):
    me = lax.axis_index("depth")
    rows = mine.shape[1]
    hops = sorted(range(1, n), key=lambda h: min(h, n - h)) + [0]

    def at_hop(h):
        return lax.rem(me + h, n)

    def span(d):
        return pl.ds(pl.multiple_of(d * rows, BLOCK), rows)

    loads = []
    for i, h in enumerate(hops):
        dest = span(at_hop(h))
        pair = (
            pltpu.make_async_copy(emis_hbm.at[:, dest, :], emis.at[i], in_sem.at[2 * i]),
            pltpu.make_async_copy(bins_hbm.at[:, dest, :], bins.at[i], in_sem.at[2 * i + 1]),
        )
        for c in pair:
            c.start()
        loads.append(pair)

    barrier = pltpu.get_barrier_semaphore()
    for h in range(1, n):
        pl.semaphore_signal(barrier, inc=1, device_id={"depth": at_hop(h)}, device_id_type=MESH)

    tables = scaled_tables(table_ref, ray_step)
    sends = []
    for i, h in enumerate(hops):
        for c in loads[i]:
            c.wait()
        for r in range(0, rows, BLOCK):
            part = march(tables, emis.at[i], bins.at[i], r)
            for c in range(4):
                if h == 0:
                    arrived[me, c, pl.ds(r, BLOCK), :] = part[c]
                else:
                    outgoing[i, c, pl.ds(r, BLOCK), :] = part[c]
        if h != 0:
            if i == 0:
                pl.semaphore_wait(barrier, n - 1)
            copy = pltpu.make_async_remote_copy(
                src_ref=outgoing.at[i],
                dst_ref=arrived.at[me],
                send_sem=send_sem.at[i],
                recv_sem=recv_sem.at[i],
                device_id={"depth": at_hop(h)},
                device_id_type=MESH,
            )
            copy.start()
            sends.append(copy)
    for copy in sends:
        copy.wait_recv()

    for r in range(0, rows, BLOCK):
        at = pl.ds(r, BLOCK)
        first = order_ref[0]
        color = [arrived[first, c, at, :] for c in range(3)]
        through = arrived[first, 3, at, :]
        for k in range(1, n):
            b = order_ref[k]
            color = [color[c] + through * arrived[b, c, at, :] for c in range(3)]
            through = through * arrived[b, 3, at, :]
        for c in range(3):
            mine[c, at, :] = color[c]
        mine[3, at, :] = 1.0 - through

    gives = []
    for i, h in enumerate(hops[:-1]):
        copy = pltpu.make_async_remote_copy(
            src_ref=mine,
            dst_ref=out_ref.at[:, span(me), :],
            send_sem=give_sem.at[i],
            recv_sem=take_sem.at[i],
            device_id={"depth": at_hop(h)},
            device_id_type=MESH,
        )
        copy.start()
        gives.append(copy)
    out_ref[:, span(me), :] = mine[...]
    for copy in sends:
        copy.wait_send()
    for copy in gives:
        copy.wait()


def fused_call(emissivity, bin_index, color_table, brick_order, n, ray_step):
    cells, cols_x, cols_y = emissivity.shape
    rows = cols_x // n
    return pl.pallas_call(
        functools.partial(fused, n, ray_step),
        out_shape=pltpu.VMEM((4, cols_x, cols_y), jnp.float32),
        in_specs=[
            pl.BlockSpec(memory_space=pltpu.HBM),
            pl.BlockSpec(memory_space=pltpu.HBM),
            pl.BlockSpec(memory_space=pltpu.VMEM),
            pl.BlockSpec(memory_space=pltpu.SMEM),
        ],
        out_specs=pl.BlockSpec(memory_space=pltpu.VMEM),
        scratch_shapes=[
            pltpu.VMEM((n, cells, rows, cols_y), jnp.bfloat16),
            pltpu.VMEM((n, cells, rows, cols_y), jnp.int32),
            pltpu.VMEM((n - 1, 4, rows, cols_y), jnp.float32),
            pltpu.VMEM((n, 4, rows, cols_y), jnp.float32),
            pltpu.VMEM((4, rows, cols_y), jnp.float32),
            pltpu.SemaphoreType.DMA((2 * n,)),
            pltpu.SemaphoreType.DMA((n - 1,)),
            pltpu.SemaphoreType.DMA((n - 1,)),
            pltpu.SemaphoreType.DMA((n - 1,)),
            pltpu.SemaphoreType.DMA((n - 1,)),
        ],
        compiler_params=pltpu.CompilerParams(collective_id=0, has_side_effects=True),
    )(emissivity, bin_index, color_table, brick_order)


def march_kernel(ray_step, emis_ref, bins_ref, table_ref, out_ref):
    tables = scaled_tables(table_ref, ray_step)

    @pl.loop(0, emis_ref.shape[1] // BLOCK)
    def _(r):
        start = pl.multiple_of(r * BLOCK, BLOCK)
        part = march(tables, emis_ref, bins_ref, start)
        for c in range(4):
            out_ref[c, pl.ds(start, BLOCK), :] = part[c]


def spread(emissivity, bin_index, color_table, brick_order, n, ray_step):
    cells, cols_x, cols_y = emissivity.shape
    piece_len = cols_x * cols_y // n
    stacked = pl.pallas_call(
        functools.partial(march_kernel, ray_step),
        out_shape=jax.ShapeDtypeStruct((4, cols_x, cols_y), jnp.float32),
        in_specs=[pl.BlockSpec(memory_space=pltpu.VMEM)] * 3,
        out_specs=pl.BlockSpec(memory_space=pltpu.VMEM),
    )(emissivity, bin_index, color_table)
    stacked = stacked.reshape(1, 4, n, piece_len).transpose(2, 0, 1, 3).reshape(n, 4, piece_len)
    received = lax.all_to_all(stacked, "depth", split_axis=0, concat_axis=0, tiled=True)
    ordered = jnp.take(received, brick_order, axis=0)
    color, through = ordered[0, 0:3], ordered[0, 3]
    for k in range(1, n):
        color = color + through * ordered[k, 0:3]
        through = through * ordered[k, 3]
    piece = jnp.concatenate([color, (1.0 - through)[None]], 0)
    return lax.all_gather(piece, "depth", axis=1, tiled=True).reshape(4, cols_x, cols_y)


def on_device(emissivity, bin_index, color_table, brick_order):
    cells, cols_x, cols_y = emissivity.shape
    n = lax.axis_size("depth")
    ray_step = 2.0 / (cells * n)
    piecewise = cols_x % (n * BLOCK) == 0
    form = fused_call if piecewise else spread
    return form(emissivity, bin_index, color_table, brick_order, n, ray_step)


def solution(mesh):
    return jax.shard_map(
        on_device,
        mesh=mesh,
        in_specs=(P("depth", "imgx", "imgy"), P("depth", "imgx", "imgy"), P(), P()),
        out_specs=P(None, "imgx", "imgy"),
        check_vma=False,
    )
```
